32 devices in a mesh: aa: 8 (over y, x, core), ba: 4 (over z).
Axes of the slice: x: 2, y: 2, z: 4, core: 2. Of those that a mesh axis runs over, the one named last changes fastest.
Arguments:
- queries: bfloat16 [4, 128, 8192], P('ba', None, 'aa'), may hold values from -10 to 10
- new_kv: bfloat16 [4, 128, 2, 512], P('ba', 'aa'), may hold values from -4 to 4
- pool: bfloat16 [4, 64, 32, 2, 512], P('ba', 'aa'), may hold values from -4 to 4
- page_table: int32 [4, 32], P('ba', 'aa'), may hold values from 0 to 7, as said below
- ctx_len: int32 [4, 8], P('ba', 'aa'), may hold values from 1 to 128, as said below
- move_page: int32 [4, 24], P('ba', 'aa'), may hold values from 0 to 7, as said below
- move_dest: int32 [4, 24], P('ba', 'aa'), may hold values from 0 to 3, as said below
- append_page: int32 [4, 8], P('ba', 'aa'), may hold values from 0 to 7
Outputs:
- attended: bfloat16 [4, 128, 8192], P('ba', None, 'aa')
- pool_out: bfloat16 [4, 64, 32, 2, 512], P('ba', 'aa')
The draws below stay inside these ranges and needn't reach their ends.
Inputs may be any that keep to these rules, and one draw needn't show every extreme that they name: `page_table`: the entries of one device are distinct pages of its pool and differ from its leaving pages and its append page. `ctx_len`: for each instance some index of aa holds exactly 128 live rows. `move_page`: the 3 entries of one device are distinct pages of its pool. `move_dest`: A device never names its own instance and names any one instance at most 2 times; for each index of aa one instance is named exactly 2 times by the device of every other instance.
All inputs are finite; a program needn't handle non-finite values.
Results may differ from the reference program's by a relative error of at most 0.0017.
Values may be sent and summed in bfloat16 or wider, within the bound.
A program may use at most 64 MiB of HBM per device.

```python
import math
import jax
import jax.numpy as jnp
from jax import lax

HEADS = 64
KV_HEADS = 4
HEAD_DIM = 128
PAGE = 32
MOST = 2
NEW_ROWS = 128
TABLE = 4
GROUP = 16
INSTANCES = 4
MOVES = 3
POOL = 8
NEW_DEV = 16
N_AA = 8


def draw_new_kv(key, part):
    out_shape = (INSTANCES, NEW_ROWS, 2, KV_HEADS * HEAD_DIM)
    values = jnp.clip(jax.random.normal(jax.random.fold_in(key, 71), out_shape, jnp.float32), -4.0, 4.0)
    return values.astype(jnp.bfloat16)


def draw_queries(key, part):
    out_shape = (INSTANCES, NEW_ROWS, HEADS * HEAD_DIM)
    drawn = 2.5 * jax.random.normal(jax.random.fold_in(key, 75), out_shape, jnp.float32)
    return jnp.clip(drawn, -10.0, 10.0).astype(jnp.bfloat16)


def shuffle_pages(sub_key):
    return jax.random.permutation(sub_key, POOL).astype(jnp.int32)


def page_lists(key):
    sub_keys = jax.random.split(jax.random.fold_in(key, 31), INSTANCES * N_AA)
    orders = jax.vmap(shuffle_pages)(sub_keys)
    return orders.reshape(INSTANCES, N_AA, POOL)


def draw_page_table(key, part):
    return page_lists(key)[:, :, :TABLE].reshape(INSTANCES, N_AA * TABLE)


def draw_move_page(key, part):
    return page_lists(key)[:, :, TABLE:TABLE + MOVES].reshape(INSTANCES, N_AA * MOVES)


def draw_append_page(key, part):
    return page_lists(key)[:, :, TABLE + MOVES]


def shuffle_slots(sub_key):
    return jax.random.permutation(sub_key, (INSTANCES - 1) * MOST).astype(jnp.int32)


def draw_move_dest(key, part):
    seeded = jax.random.fold_in(key, 37)
    option_count = (INSTANCES - 1) * MOST
    busiest = jax.random.randint(jax.random.fold_in(seeded, 1), (N_AA,), 0, INSTANCES)
    source = jnp.arange(INSTANCES)[:, None]
    candidate = (source + 1 + jnp.arange(option_count)[None, :] // MOST) % INSTANCES
    sub_keys = jax.random.split(jax.random.fold_in(seeded, 2), INSTANCES * N_AA)
    scores = jax.vmap(shuffle_slots)(sub_keys).reshape(INSTANCES, N_AA, option_count)
    forced = candidate[:, None, :] == busiest[None, :, None]
    priority = jnp.where(forced, scores + option_count, scores)
    picked = lax.top_k(priority, MOVES)[1]
    spread = jnp.broadcast_to(candidate[:, None, :], priority.shape)
    chosen_dest = jnp.take_along_axis(spread, picked, axis=-1)
    return chosen_dest.reshape(INSTANCES, N_AA * MOVES).astype(jnp.int32)


def draw_ctx_len(key, part):
    seeded = jax.random.fold_in(key, 41)
    full_rows = TABLE * PAGE
    lengths = jax.random.randint(jax.random.fold_in(seeded, 1), (INSTANCES, N_AA), 1, full_rows + 1)
    full_index = jax.random.randint(jax.random.fold_in(seeded, 2), (INSTANCES,), 0, N_AA)
    hit_full = jnp.arange(N_AA)[None, :] == full_index[:, None]
    return jnp.where(hit_full, full_rows, lengths).astype(jnp.int32)


def shard_levels(own_key, dims, shards, smallest, top_value):
    level = 1.0
    for dim, parts in shards:
        steps = jax.random.uniform(jax.random.fold_in(jax.random.fold_in(own_key, 6), dim), (parts,), jnp.float32, smallest / len(shards), top_value / len(shards))
        level = level * jnp.repeat(jnp.exp(steps), dims[dim] // parts).reshape((-1,) + (1,) * (len(dims) - 1 - dim))
    return level


def scatter_about(key, shape, scale, most, cuts=(), kind=jnp.bfloat16):
    level = shard_levels(key, shape, cuts, -0.22, 0.18) if cuts else 1.0
    values = jax.random.normal(key, shape, jnp.float32) * scale * level
    return jnp.minimum(jnp.maximum(values, -most), most).astype(kind)


def setup_inputs(seed: int = 0) -> dict:
    key_list = jax.random.split(jax.random.key(seed), 9)
    queries = draw_queries(jax.random.fold_in(key_list[8], 71), 0)
    new_kv = draw_new_kv(jax.random.fold_in(key_list[8], 71), 0)
    pool = scatter_about(key_list[2], (INSTANCES, N_AA * POOL, PAGE, 2, KV_HEADS * HEAD_DIM), 1.0, 4.0, ((0, 4), (1, 8)))
    page_table = draw_page_table(jax.random.fold_in(key_list[8], 71), 0)
    ctx_len = draw_ctx_len(jax.random.fold_in(key_list[8], 71), 0)
    move_page = draw_move_page(jax.random.fold_in(key_list[8], 71), 0)
    move_dest = draw_move_dest(jax.random.fold_in(key_list[8], 71), 0)
    append_page = draw_append_page(jax.random.fold_in(key_list[8], 71), 0)
    return dict(queries=queries, new_kv=new_kv, pool=pool, page_table=page_table, ctx_len=ctx_len, move_page=move_page, move_dest=move_dest, append_page=append_page)


def pick_pages(pages, page_ids):
    return jnp.take(pages, page_ids.astype(jnp.int32), axis=0)

def place_rows(pages, fresh_rows, page_id):
    start = page_id.astype(jnp.int32)
    zero = jnp.zeros((), jnp.int32)
    return lax.dynamic_update_slice(pages, fresh_rows[None], (start, zero, zero, zero))

def attention(query_rows, key_rows, visible):
    query_heads = query_rows.astype(jnp.float32).reshape(NEW_ROWS, KV_HEADS, GROUP, HEAD_DIM).transpose(1, 0, 2, 3)
    head_keys = key_rows[:, 0].astype(jnp.float32).reshape(-1, KV_HEADS, HEAD_DIM).transpose(1, 0, 2)
    head_values = key_rows[:, 1].astype(jnp.float32).reshape(-1, KV_HEADS, HEAD_DIM).transpose(1, 0, 2)

    def one_head(operands):
        head_query, key_block, value_block = operands
        scores = jnp.einsum('qgd,rd->qgr', head_query, key_block) / math.sqrt(HEAD_DIM)
        scores = jnp.where(visible[:, None, :], scores, -jnp.inf)
        row_top = lax.optimization_barrier(jnp.max(scores, axis=-1, keepdims=True))
        weights = jnp.exp(scores - row_top)
        row_total = lax.optimization_barrier(jnp.sum(weights, axis=-1))
        return jnp.einsum('qgr,rd->qgd', weights, value_block, precision=lax.Precision.HIGHEST) / row_total[..., None]
    outputs = lax.map(one_head, (query_heads, head_keys, head_values))
    return outputs.transpose(1, 0, 2, 3).reshape(NEW_ROWS, HEADS * HEAD_DIM).astype(jnp.bfloat16)

def reference(queries, new_kv, pool, page_table, ctx_len, move_page, move_dest, append_page):
    kv_width = KV_HEADS * HEAD_DIM
    pool_pages = pool.reshape(INSTANCES, N_AA, POOL, PAGE, 2, kv_width)
    tables = page_table.reshape(INSTANCES, N_AA, TABLE)
    moved_ids = move_page.reshape(INSTANCES, N_AA, MOVES)
    targets = move_dest.reshape(INSTANCES, N_AA, MOVES)
    counter = jnp.arange(MOVES, dtype=jnp.int32)
    earlier = counter[None, :] < counter[:, None]
    same_target = targets[..., :, None] == targets[..., None, :]
    ranks = lax.optimization_barrier(jnp.sum(same_target & earlier, axis=-1)).astype(jnp.int32)
    pick_all = jax.vmap(jax.vmap(pick_pages))
    slot_numbers = jnp.arange(MOST, dtype=jnp.int32)
    row_offsets = jnp.arange(TABLE * PAGE, dtype=jnp.int32)
    causal = jnp.arange(NEW_ROWS, dtype=jnp.int32)[None, :] <= jnp.arange(NEW_ROWS, dtype=jnp.int32)[:, None]

    def serve_instance(target):
        slot_hit = (targets == target)[..., None] & (ranks[..., None] == slot_numbers)
        page_ids = lax.optimization_barrier(jnp.sum(jnp.where(slot_hit, moved_ids[..., None], 0), axis=2)).astype(jnp.int32)
        arrived = jnp.any(slot_hit, axis=2)
        moved_rows = pick_all(pool_pages, page_ids).reshape(-1, 2, kv_width)
        moved_live = jnp.broadcast_to(arrived[..., None], (INSTANCES, N_AA, MOST, PAGE)).reshape(-1)
        own_pages = lax.dynamic_index_in_dim(pool_pages, target, 0, keepdims=False)
        own_table = lax.dynamic_index_in_dim(tables, target, 0, keepdims=False)
        own_rows = jax.vmap(pick_pages)(own_pages, own_table).reshape(-1, 2, kv_width)
        lengths = lax.dynamic_index_in_dim(ctx_len, target, 0, keepdims=False)
        own_live = (row_offsets[None, :] < lengths[:, None]).reshape(-1)
        fresh_rows = lax.dynamic_index_in_dim(new_kv, target, 0, keepdims=False)
        key_rows = jnp.concatenate([own_rows, moved_rows, fresh_rows], axis=0)
        visible = jnp.concatenate([jnp.broadcast_to(own_live[None, :], (NEW_ROWS, own_live.shape[0])), jnp.broadcast_to(moved_live[None, :], (NEW_ROWS, moved_live.shape[0])), causal], axis=1)
        query_rows = lax.dynamic_index_in_dim(queries, target, 0, keepdims=False)
        return attention(query_rows, key_rows, visible)
    attended = lax.map(serve_instance, jnp.arange(INSTANCES, dtype=jnp.int32))
    fresh_all = new_kv.reshape(INSTANCES, N_AA, NEW_DEV, 2, kv_width)
    updated = jax.vmap(jax.vmap(place_rows))(pool_pages, fresh_all, append_page)
    return (attended, updated.reshape(pool.shape))
```

```python
import functools
import math

import jax
import jax.numpy as jnp
from jax import lax
from jax.experimental import pallas as pl
from jax.experimental.pallas import tpu as pltpu
from jax.sharding import PartitionSpec as P

HEAD_DIM = 128
MOST = 2
LANES = 128
NEG_LARGE = -1e30
MESH = pl.DeviceIdType.MESH


def kernel(
    n_inst, n_aa, kv_heads,
    table_ref, len_ref, page_ref, dest_ref, q_ref, pages_ref, fresh_ref,
    out_ref,
    st_res, st_mov, st_len, st_occ,
    kv_res, kv_new, kv_mov, len_all, occ_all,
    run_max, run_sum, run_out,
    s_res, r_res, s_new, r_new, s_mov, r_mov, s_len, r_len, s_occ, r_occ,
    fs_res, fr_res, fs_new, fr_new, fs_mov, fr_mov, fs_len, fr_len, fs_occ, fr_occ,
    l_new, l_res,
):
    b = lax.axis_index("ba")
    a = lax.axis_index("aa")
    share = n_aa // kv_heads
    mine, member = a // share, a % share
    table = table_ref.shape[1]
    moves = page_ref.shape[1]
    page_rows = pages_ref.shape[3]
    queries = q_ref.shape[0]
    heads = q_ref.shape[1] // HEAD_DIM

    def inst(r):
        return lax.rem(b + r + n_inst, n_inst)

    def at_head(j):
        return lax.rem(mine + j + kv_heads, kv_heads) * share + member

    def peer(k):
        return mine * share + lax.rem(member + k + share, share)

    barrier = pltpu.get_barrier_semaphore()
    partners = [(r, j) for r in range(n_inst) for j in range(kv_heads) if r or j]
    for r, j in partners:
        pl.semaphore_signal(barrier, inc=1, device_id={"ba": inst(r), "aa": at_head(j)}, device_id_type=MESH)
    for k in range(1, share):
        pl.semaphore_signal(barrier, inc=1, device_id={"ba": b, "aa": peer(k)}, device_id_type=MESH)

    lane = lax.broadcasted_iota(jnp.int32, (8, LANES), 1)
    for r in range(1, n_inst):
        target = inst(r)
        slot_bias = []
        for m in range(MOST):
            chosen, occupied, seen = jnp.int32(0), jnp.int32(0), jnp.int32(0)
            for i in range(moves):
                hit = (dest_ref[0, i] == target).astype(jnp.int32)
                here = hit * (seen == m).astype(jnp.int32)
                chosen = chosen + here * page_ref[0, i]
                occupied = occupied + here
                seen = seen + hit
            st_mov[r - 1, :, :, m * page_rows:(m + 1) * page_rows, :] = pages_ref[chosen]
            slot_bias.append(jnp.where(occupied > 0, 0.0, NEG_LARGE))
        row = jnp.full((8, LANES), slot_bias[0], jnp.float32)
        for m in range(1, MOST):
            row = jnp.where((lane // page_rows) % MOST == m, slot_bias[m], row)
        st_occ[r - 1] = row
    for j in range(table):
        st_res[:, :, j * page_rows:(j + 1) * page_rows, :] = pages_ref[table_ref[0, j]]
    place = lax.broadcasted_iota(jnp.int32, st_len.shape, 1)
    st_len[...] = jnp.where(place < len_ref[0, 0], 0.0, NEG_LARGE)
    len_all[a] = st_len[...]

    pl.semaphore_wait(barrier, len(partners) + share - 1)

    def remote(src, dst, ss, rs, ba, aa):
        return pltpu.make_async_remote_copy(
            src_ref=src, dst_ref=dst, send_sem=ss, recv_sem=rs,
            device_id={"ba": ba, "aa": aa}, device_id_type=MESH,
        )

    sent = []

    def start(*args):
        c = remote(*args)
        c.start()
        sent.append(c)

    for r in range(1, n_inst):
        for j in range(kv_heads):
            to = at_head(j)
            h = lax.rem(mine + j, kv_heads)
            start(st_mov.at[r - 1, h], kv_mov.at[r - 1, a], s_mov.at[r - 1, j], r_mov.at[r - 1, j], inst(r), to)
            start(st_occ.at[r - 1], occ_all.at[r - 1, a], s_occ.at[r - 1, j], r_occ.at[r - 1, j], inst(r), to)
        if r == 1:
            for j in range(1, kv_heads):
                to = at_head(j)
                h = lax.rem(mine + j, kv_heads)
                start(fresh_ref.at[h], kv_new.at[a], s_new.at[j], r_new.at[j], b, to)
                start(st_len, len_all.at[a], s_len.at[j], r_len.at[j], b, to)
                start(st_res.at[h], kv_res.at[a], s_res.at[j], r_res.at[j], b, to)
            for k in range(1, share):
                to = peer(k)
                start(fresh_ref.at[mine], kv_new.at[a], fs_new.at[k - 1, 0], fr_new.at[k - 1, 0], b, to)
                start(st_len, len_all.at[a], fs_len.at[k - 1, 0], fr_len.at[k - 1, 0], b, to)
                start(st_res.at[mine], kv_res.at[a], fs_res.at[k - 1, 0], fr_res.at[k - 1, 0], b, to)
    own_new = pltpu.make_async_copy(fresh_ref.at[mine], kv_new.at[a], l_new)
    own_new.start()
    own_res = pltpu.make_async_copy(st_res.at[mine], kv_res.at[a], l_res)
    own_res.start()

    def arrived(slot, rs, ss):
        remote(slot, slot, ss, rs, b, a).wait_recv()

    def relay(slot, rs, ss, fs, fr, j):
        arrived(slot, rs, ss)
        for k in range(1, share):
            start(slot, slot, fs.at[k - 1, j], fr.at[k - 1, j], b, peer(k))

    def peers_done(buf, fs, fr, first=0):
        for k in range(1, share):
            for j in range(kv_heads):
                src = lax.rem(mine - j + kv_heads, kv_heads) * share + lax.rem(member - k + share, share)
                arrived(buf.at[src], fr.at[k - 1, j], fs.at[k - 1, j])

    for j in range(1, kv_heads):
        src = at_head(-j)
        relay(kv_new.at[src], r_new.at[j], s_new.at[j], fs_new, fr_new, j)
        relay(len_all.at[src], r_len.at[j], s_len.at[j], fs_len, fr_len, j)
        relay(kv_res.at[src], r_res.at[j], s_res.at[j], fs_res, fr_res, j)

    scale = math.log2(math.e) / math.sqrt(HEAD_DIM)

    def attend(keys, values, bias, first):
        def one_head(h, carry):
            q = q_ref[:, pl.ds(pl.multiple_of(h * HEAD_DIM, HEAD_DIM), HEAD_DIM)]
            s = lax.dot_general(q, keys(), (((1,), (1,)), ((), ())), preferred_element_type=jnp.float32)
            s = s * scale + bias
            top = jnp.max(s, axis=1, keepdims=True)
            if not first:
                old = run_max[h]
                top = jnp.maximum(old, top)
            w = jnp.exp2(s - top)
            total = jnp.sum(w, axis=1, keepdims=True)
            high = w.astype(jnp.bfloat16)
            low = (w - high.astype(jnp.float32)).astype(jnp.bfloat16)
            v = values()
            out = jnp.dot(high, v, preferred_element_type=jnp.float32)
            out = out + jnp.dot(low, v, preferred_element_type=jnp.float32)
            if not first:
                shrink = jnp.exp2(old - top)
                total = total + run_sum[h] * shrink
                out = out + run_out[h] * shrink
            run_max[h] = top
            run_sum[h] = total
            run_out[h] = out
            return carry
        lax.fori_loop(0, heads, one_head, 0)

    own_new.wait()
    peers_done(kv_new, fs_new, fr_new)
    rows = lax.broadcasted_iota(jnp.int32, (queries, queries), 0)
    columns = lax.broadcasted_iota(jnp.int32, (queries, queries), 1)
    attend(
        lambda: kv_new[:, 0].reshape(-1, HEAD_DIM),
        lambda: kv_new[:, 1].reshape(-1, HEAD_DIM),
        jnp.where(columns <= rows, 0.0, NEG_LARGE),
        True,
    )
    own_res.wait()
    peers_done(len_all, fs_len, fr_len)
    peers_done(kv_res, fs_res, fr_res)
    attend(
        lambda: kv_res[:, 0].reshape(-1, HEAD_DIM),
        lambda: kv_res[:, 1].reshape(-1, HEAD_DIM),
        jnp.concatenate([len_all[i, 0:1, :] for i in range(n_aa)], axis=1),
        False,
    )
    packed = LANES // (MOST * page_rows)
    lane1 = lax.broadcasted_iota(jnp.int32, (1, LANES), 1)
    for r in range(1, n_inst):
        for j in range(kv_heads):
            src = at_head(-j)
            relay(kv_mov.at[r - 1, src], r_mov.at[r - 1, j], s_mov.at[r - 1, j], fs_mov.at[r - 1], fr_mov.at[r - 1], j)
            relay(occ_all.at[r - 1, src], r_occ.at[r - 1, j], s_occ.at[r - 1, j], fs_occ.at[r - 1], fr_occ.at[r - 1], j)
        peers_done(kv_mov.at[r - 1], fs_mov.at[r - 1], fr_mov.at[r - 1])
        peers_done(occ_all.at[r - 1], fs_occ.at[r - 1], fr_occ.at[r - 1])
        pieces = []
        for g in range(n_aa // packed):
            piece = occ_all[r - 1, g * packed, 0:1, :]
            for i in range(1, packed):
                piece = jnp.where(lane1 >= i * MOST * page_rows, occ_all[r - 1, g * packed + i, 0:1, :], piece)
            pieces.append(piece)
        attend(
            lambda: kv_mov[r - 1, :, 0].reshape(-1, HEAD_DIM),
            lambda: kv_mov[r - 1, :, 1].reshape(-1, HEAD_DIM),
            jnp.concatenate(pieces, axis=1),
            False,
        )
    for h in range(heads):
        out_ref[:, h * HEAD_DIM:(h + 1) * HEAD_DIM] = (run_out[h] / run_sum[h]).astype(out_ref.dtype)
    for c in sent:
        c.wait_send()


def local(n_inst, n_aa, queries, new_kv, pool, page_table, ctx_len, move_page, move_dest, append_page):
    pool_pages = pool[0]
    pages, page_rows, _, width = pool_pages.shape
    kv_heads = width // HEAD_DIM
    share = n_aa // kv_heads
    fresh_rows = new_kv[0]
    fresh_count = fresh_rows.shape[0]
    split = pool_pages.reshape(pages, page_rows, 2, kv_heads, HEAD_DIM).transpose(0, 3, 2, 1, 4)
    fresh = fresh_rows.reshape(fresh_count, 2, kv_heads, HEAD_DIM).transpose(2, 1, 0, 3)
    query_count, q_width = queries.shape[1:]
    heads = q_width // HEAD_DIM
    table = page_table.shape[1]
    far = n_inst - 1
    bf, f32 = jnp.bfloat16, jnp.float32
    dma = pltpu.SemaphoreType.DMA
    near = [dma((kv_heads,))] * 4
    attended = pl.pallas_call(
        functools.partial(kernel, n_inst, n_aa, kv_heads),
        out_shape=jax.ShapeDtypeStruct((query_count, q_width), bf),
        in_specs=[pl.BlockSpec(memory_space=pltpu.SMEM)] * 4 + [pl.BlockSpec(memory_space=pltpu.VMEM)] * 3,
        out_specs=pl.BlockSpec(memory_space=pltpu.VMEM),
        scratch_shapes=[
            pltpu.VMEM((kv_heads, 2, table * page_rows, HEAD_DIM), bf),
            pltpu.VMEM((far, kv_heads, 2, MOST * page_rows, HEAD_DIM), bf),
            pltpu.VMEM((8, table * page_rows), f32),
            pltpu.VMEM((far, 8, LANES), f32),
            pltpu.VMEM((n_aa, 2, table * page_rows, HEAD_DIM), bf),
            pltpu.VMEM((n_aa, 2, fresh_count, HEAD_DIM), bf),
            pltpu.VMEM((far, n_aa, 2, MOST * page_rows, HEAD_DIM), bf),
            pltpu.VMEM((n_aa, 8, table * page_rows), f32),
            pltpu.VMEM((far, n_aa, 8, LANES), f32),
            pltpu.VMEM((heads, query_count, 1), f32),
            pltpu.VMEM((heads, query_count, 1), f32),
            pltpu.VMEM((heads, query_count, HEAD_DIM), f32),
            *near,
            dma((far, kv_heads)), dma((far, kv_heads)),
            dma((kv_heads,)), dma((kv_heads,)),
            dma((far, kv_heads)), dma((far, kv_heads)),
            *([dma((share - 1, kv_heads))] * 4),
            dma((far, share - 1, kv_heads)), dma((far, share - 1, kv_heads)),
            dma((share - 1, kv_heads)), dma((share - 1, kv_heads)),
            dma((far, share - 1, kv_heads)), dma((far, share - 1, kv_heads)),
            dma, dma,
        ],
        compiler_params=pltpu.CompilerParams(collective_id=0, has_side_effects=True),
        name="paged_attention",
    )(page_table, ctx_len, move_page, move_dest, queries[0], split, fresh)
    zero = jnp.zeros((), jnp.int32)
    updated = lax.dynamic_update_slice(pool_pages, fresh_rows[None], (append_page[0, 0], zero, zero, zero))
    return (attended[None], updated[None])


def solution(mesh):
    return jax.shard_map(
        functools.partial(local, mesh.shape["ba"], mesh.shape["aa"]),
        mesh=mesh,
        in_specs=(
            P("ba", None, "aa"),
            P("ba", "aa", None, None),
            P("ba", "aa", None, None, None),
            P("ba", "aa"),
            P("ba", "aa"),
            P("ba", "aa"),
            P("ba", "aa"),
            P("ba", "aa"),
        ),
        out_specs=(P("ba", None, "aa"), P("ba", "aa", None, None, None)),
        check_vma=False,
    )
```

```python
import functools
import math

import jax
import jax.numpy as jnp
from jax import lax
from jax.experimental import pallas as pl
from jax.experimental.pallas import tpu as pltpu
from jax.sharding import PartitionSpec as P

HEAD_DIM = 128
MOST = 2
LANES = 128
BLOCK = 256
NEG_LARGE = -1e30
MESH = pl.DeviceIdType.MESH


def kernel(
    n_inst, n_aa, kv_heads,
    table_ref, len_ref, page_ref, dest_ref, q_ref, pages_ref, fresh_ref,
    out_ref,
    st_res, st_mov, st_len, st_occ,
    kv_res, kv_new, kv_mov, len_all, occ_all,
    run_max, run_sum, run_out, q_turned,
    s_res, r_res, s_new, r_new, s_mov, r_mov, s_len, r_len, s_occ, r_occ,
    fs_res, fr_res, fs_new, fr_new, fs_mov, fr_mov, fs_len, fr_len, fs_occ, fr_occ,
    l_new, l_res,
):
    b = lax.axis_index("ba")
    a = lax.axis_index("aa")
    share = n_aa // kv_heads
    mine, member = a // share, a % share
    table = table_ref.shape[1]
    moves = page_ref.shape[1]
    page_rows = pages_ref.shape[3]
    queries = q_ref.shape[0]
    heads = q_ref.shape[1] // HEAD_DIM

    def inst(r):
        return lax.rem(b + r + n_inst, n_inst)

    def at_head(j):
        return lax.rem(mine + j + kv_heads, kv_heads) * share + member

    def peer(k):
        return mine * share + lax.rem(member + k + share, share)

    barrier = pltpu.get_barrier_semaphore()
    partners = [(r, j) for r in range(n_inst) for j in range(kv_heads) if r or j]
    for r, j in partners:
        pl.semaphore_signal(barrier, inc=1, device_id={"ba": inst(r), "aa": at_head(j)}, device_id_type=MESH)
    for k in range(1, share):
        pl.semaphore_signal(barrier, inc=1, device_id={"ba": b, "aa": peer(k)}, device_id_type=MESH)

    line = lax.broadcasted_iota(jnp.int32, (8, LANES), 0)
    for r in range(1, n_inst):
        target = inst(r)
        slot_bias = []
        for m in range(MOST):
            chosen, occupied, seen = jnp.int32(0), jnp.int32(0), jnp.int32(0)
            for i in range(moves):
                hit = (dest_ref[0, i] == target).astype(jnp.int32)
                here = hit * (seen == m).astype(jnp.int32)
                chosen = chosen + here * page_ref[0, i]
                occupied = occupied + here
                seen = seen + hit
            st_mov[r - 1, :, :, m * page_rows:(m + 1) * page_rows, :] = pages_ref[chosen]
            slot_bias.append(jnp.where(occupied > 0, 0.0, NEG_LARGE))
        row = jnp.full((8, LANES), slot_bias[0], jnp.float32)
        for m in range(1, MOST):
            row = jnp.where(line == m, slot_bias[m], row)
        st_occ[r - 1] = row
    for j in range(table):
        st_res[:, :, j * page_rows:(j + 1) * page_rows, :] = pages_ref[table_ref[0, j]]
    st_len[...] = jnp.full(st_len.shape, len_ref[0, 0], jnp.int32)
    len_all[a] = st_len[...]
    for h in range(heads):
        q_turned[:, h * queries:(h + 1) * queries] = q_ref[:, h * HEAD_DIM:(h + 1) * HEAD_DIM].T

    pl.semaphore_wait(barrier, len(partners) + share - 1)

    def remote(src, dst, ss, rs, ba, aa):
        return pltpu.make_async_remote_copy(
            src_ref=src, dst_ref=dst, send_sem=ss, recv_sem=rs,
            device_id={"ba": ba, "aa": aa}, device_id_type=MESH,
        )

    sent = []

    def start(*args):
        c = remote(*args)
        c.start()
        sent.append(c)

    for r in range(1, n_inst):
        for j in range(kv_heads):
            to = at_head(j)
            h = lax.rem(mine + j, kv_heads)
            start(st_mov.at[r - 1, h], kv_mov.at[r - 1, a], s_mov.at[r - 1, j], r_mov.at[r - 1, j], inst(r), to)
            start(st_occ.at[r - 1], occ_all.at[r - 1, a], s_occ.at[r - 1, j], r_occ.at[r - 1, j], inst(r), to)
        if r == 1:
            for j in range(1, kv_heads):
                to = at_head(j)
                h = lax.rem(mine + j, kv_heads)
                start(fresh_ref.at[h], kv_new.at[a], s_new.at[j], r_new.at[j], b, to)
                start(st_len, len_all.at[a], s_len.at[j], r_len.at[j], b, to)
                start(st_res.at[h], kv_res.at[a], s_res.at[j], r_res.at[j], b, to)
            for k in range(1, share):
                to = peer(k)
                start(fresh_ref.at[mine], kv_new.at[a], fs_new.at[k - 1, 0], fr_new.at[k - 1, 0], b, to)
                start(st_len, len_all.at[a], fs_len.at[k - 1, 0], fr_len.at[k - 1, 0], b, to)
                start(st_res.at[mine], kv_res.at[a], fs_res.at[k - 1, 0], fr_res.at[k - 1, 0], b, to)
    own_new = pltpu.make_async_copy(fresh_ref.at[mine], kv_new.at[a], l_new)
    own_new.start()
    own_res = pltpu.make_async_copy(st_res.at[mine], kv_res.at[a], l_res)
    own_res.start()

    def arrived(slot, rs, ss):
        remote(slot, slot, ss, rs, b, a).wait_recv()

    def relay(slot, rs, ss, fs, fr, j):
        arrived(slot, rs, ss)
        for k in range(1, share):
            start(slot, slot, fs.at[k - 1, j], fr.at[k - 1, j], b, peer(k))

    def peers_done(buf, fs, fr, first=0):
        for k in range(1, share):
            for j in range(kv_heads):
                src = lax.rem(mine - j + kv_heads, kv_heads) * share + lax.rem(member - k + share, share)
                arrived(buf.at[src], fr.at[k - 1, j], fs.at[k - 1, j])

    for j in range(1, kv_heads):
        src = at_head(-j)
        relay(kv_new.at[src], r_new.at[j], s_new.at[j], fs_new, fr_new, j)
        relay(len_all.at[src], r_len.at[j], s_len.at[j], fs_len, fr_len, j)
        relay(kv_res.at[src], r_res.at[j], s_res.at[j], fs_res, fr_res, j)

    scale = math.log2(math.e) / math.sqrt(HEAD_DIM)

    def attend(keys, values, bias, first):
        turned = values.T
        copies = BLOCK // bias.shape[1]
        wide = jnp.concatenate([bias] * copies, axis=1) if copies > 1 else bias
        for start_at in range(0, heads * queries, BLOCK):
            block = slice(start_at, start_at + BLOCK)
            s = jnp.dot(keys, q_turned[:, block], preferred_element_type=jnp.float32)
            s = s * scale + wide
            top = jnp.max(s, axis=0, keepdims=True)
            if not first:
                old = run_max[:, block]
                top = jnp.maximum(old, top)
            w = jnp.exp2(s - top)
            total = jnp.sum(w, axis=0, keepdims=True)
            high = w.astype(jnp.bfloat16)
            low = (w - high.astype(jnp.float32)).astype(jnp.bfloat16)
            out = jnp.dot(turned, high, preferred_element_type=jnp.float32)
            out = out + jnp.dot(turned, low, preferred_element_type=jnp.float32)
            if not first:
                shrink = jnp.exp2(old - top)
                total = total + run_sum[:, block] * shrink
                out = out + run_out[:, block] * shrink
            run_max[:, block] = top
            run_sum[:, block] = total
            run_out[:, block] = out

    own_new.wait()
    peers_done(kv_new, fs_new, fr_new)
    rows = lax.broadcasted_iota(jnp.int32, (queries, queries), 0)
    columns = lax.broadcasted_iota(jnp.int32, (queries, queries), 1)
    attend(
        kv_new[:, 0].reshape(-1, HEAD_DIM),
        kv_new[:, 1].reshape(-1, HEAD_DIM),
        jnp.where(rows <= columns, 0.0, NEG_LARGE),
        True,
    )
    own_res.wait()
    place = lax.broadcasted_iota(jnp.int32, (table * page_rows, LANES), 0)
    peers_done(len_all, fs_len, fr_len)
    peers_done(kv_res, fs_res, fr_res)
    attend(
        kv_res[:, 0].reshape(-1, HEAD_DIM),
        kv_res[:, 1].reshape(-1, HEAD_DIM),
        jnp.concatenate([jnp.where(place < len_all[i, 0:1, :], 0.0, NEG_LARGE) for i in range(n_aa)], axis=0),
        False,
    )
    for r in range(1, n_inst):
        for j in range(kv_heads):
            src = at_head(-j)
            relay(kv_mov.at[r - 1, src], r_mov.at[r - 1, j], s_mov.at[r - 1, j], fs_mov.at[r - 1], fr_mov.at[r - 1], j)
            relay(occ_all.at[r - 1, src], r_occ.at[r - 1, j], s_occ.at[r - 1, j], fs_occ.at[r - 1], fr_occ.at[r - 1], j)
        peers_done(kv_mov.at[r - 1], fs_mov.at[r - 1], fr_mov.at[r - 1])
        peers_done(occ_all.at[r - 1], fs_occ.at[r - 1], fr_occ.at[r - 1])
        pieces = [
            jnp.broadcast_to(occ_all[r - 1, i, m:m + 1, :], (page_rows, LANES))
            for i in range(n_aa) for m in range(MOST)
        ]
        attend(
            kv_mov[r - 1, :, 0].reshape(-1, HEAD_DIM),
            kv_mov[r - 1, :, 1].reshape(-1, HEAD_DIM),
            jnp.concatenate(pieces, axis=0),
            False,
        )
    def turn(h):
        part = slice(h * queries, (h + 1) * queries)
        return (run_out[:, part] / run_sum[:, part]).T

    for h in range(heads):
        out_ref[:, h * HEAD_DIM:(h + 1) * HEAD_DIM] = turn(h).astype(out_ref.dtype)
    for c in sent:
        c.wait_send()


def local(n_inst, n_aa, queries, new_kv, pool, page_table, ctx_len, move_page, move_dest, append_page):
    pool_pages = pool[0]
    pages, page_rows, _, width = pool_pages.shape
    kv_heads = width // HEAD_DIM
    share = n_aa // kv_heads
    fresh_rows = new_kv[0]
    fresh_count = fresh_rows.shape[0]
    split = pool_pages.reshape(pages, page_rows, 2, kv_heads, HEAD_DIM).transpose(0, 3, 2, 1, 4)
    fresh = fresh_rows.reshape(fresh_count, 2, kv_heads, HEAD_DIM).transpose(2, 1, 0, 3)
    query_count, q_width = queries.shape[1:]
    heads = q_width // HEAD_DIM
    table = page_table.shape[1]
    far = n_inst - 1
    bf, f32 = jnp.bfloat16, jnp.float32
    dma = pltpu.SemaphoreType.DMA
    near = [dma((kv_heads,))] * 4
    attended = pl.pallas_call(
        functools.partial(kernel, n_inst, n_aa, kv_heads),
        out_shape=jax.ShapeDtypeStruct((query_count, q_width), bf),
        in_specs=[pl.BlockSpec(memory_space=pltpu.SMEM)] * 4 + [pl.BlockSpec(memory_space=pltpu.VMEM)] * 3,
        out_specs=pl.BlockSpec(memory_space=pltpu.VMEM),
        scratch_shapes=[
            pltpu.VMEM((kv_heads, 2, table * page_rows, HEAD_DIM), bf),
            pltpu.VMEM((far, kv_heads, 2, MOST * page_rows, HEAD_DIM), bf),
            pltpu.VMEM((8, LANES), jnp.int32),
            pltpu.VMEM((far, 8, LANES), f32),
            pltpu.VMEM((n_aa, 2, table * page_rows, HEAD_DIM), bf),
            pltpu.VMEM((n_aa, 2, fresh_count, HEAD_DIM), bf),
            pltpu.VMEM((far, n_aa, 2, MOST * page_rows, HEAD_DIM), bf),
            pltpu.VMEM((n_aa, 8, LANES), jnp.int32),
            pltpu.VMEM((far, n_aa, 8, LANES), f32),
            pltpu.VMEM((1, heads * query_count), f32),
            pltpu.VMEM((1, heads * query_count), f32),
            pltpu.VMEM((HEAD_DIM, heads * query_count), f32),
            pltpu.VMEM((HEAD_DIM, heads * query_count), bf),
            *near,
            dma((far, kv_heads)), dma((far, kv_heads)),
            dma((kv_heads,)), dma((kv_heads,)),
            dma((far, kv_heads)), dma((far, kv_heads)),
            *([dma((share - 1, kv_heads))] * 4),
            dma((far, share - 1, kv_heads)), dma((far, share - 1, kv_heads)),
            dma((share - 1, kv_heads)), dma((share - 1, kv_heads)),
            dma((far, share - 1, kv_heads)), dma((far, share - 1, kv_heads)),
            dma, dma,
        ],
        compiler_params=pltpu.CompilerParams(collective_id=0, has_side_effects=True),
        name="paged_attention",
    )(page_table, ctx_len, move_page, move_dest, queries[0], split, fresh)
    zero = jnp.zeros((), jnp.int32)
    updated = lax.dynamic_update_slice(pool_pages, fresh_rows[None], (append_page[0, 0], zero, zero, zero))
    return (attended[None], updated[None])


def solution(mesh):
    return jax.shard_map(
        functools.partial(local, mesh.shape["ba"], mesh.shape["aa"]),
        mesh=mesh,
        in_specs=(
            P("ba", None, "aa"),
            P("ba", "aa", None, None),
            P("ba", "aa", None, None, None),
            P("ba", "aa"),
            P("ba", "aa"),
            P("ba", "aa"),
            P("ba", "aa"),
            P("ba", "aa"),
        ),
        out_specs=(P("ba", None, "aa"), P("ba", "aa", None, None, None)),
        check_vma=False,
    )
```

```python
import functools
import math

import jax
import jax.numpy as jnp
from jax import lax
from jax.experimental import pallas as pl
from jax.experimental.pallas import tpu as pltpu
from jax.sharding import PartitionSpec as P

HEAD_DIM = 128
MOST = 2
LANES = 128
BLOCK = 256
NEG_LARGE = -1e30
MESH = pl.DeviceIdType.MESH


def kernel(
    n_inst, n_aa, kv_heads,
    table_ref, len_ref, page_ref, dest_ref, q_ref, pool_ref, fresh_ref,
    out_ref,
    st_res, st_new, st_mov, st_len, st_occ,
    kv_res, kv_new, kv_mov, len_all, occ_all,
    run_max, run_sum, run_out, q_turned,
    s_res, r_res, s_new, r_new, s_mov, r_mov, s_len, r_len, s_occ, r_occ,
    fs_res, fr_res, fs_new, fr_new, fs_mov, fr_mov, fs_len, fr_len, fs_occ, fr_occ,
    l_new, l_res,
):
    b = lax.axis_index("ba")
    a = lax.axis_index("aa")
    share = n_aa // kv_heads
    mine, member = a // share, a % share
    table = table_ref.shape[1]
    moves = page_ref.shape[1]
    page_rows = pool_ref.shape[1]
    queries = q_ref.shape[0]
    heads = q_ref.shape[1] // HEAD_DIM

    def inst(r):
        return lax.rem(b + r + n_inst, n_inst)

    def at_head(j):
        return lax.rem(mine + j + kv_heads, kv_heads) * share + member

    def peer(k):
        return mine * share + lax.rem(member + k + share, share)

    barrier = pltpu.get_barrier_semaphore()
    partners = [(r, j) for r in range(n_inst) for j in range(kv_heads) if r or j]
    for r, j in partners:
        pl.semaphore_signal(barrier, inc=1, device_id={"ba": inst(r), "aa": at_head(j)}, device_id_type=MESH)
    for k in range(1, share):
        pl.semaphore_signal(barrier, inc=1, device_id={"ba": b, "aa": peer(k)}, device_id_type=MESH)

    spots = [(h, w) for h in range(kv_heads) for w in range(2)]

    def columns_of(h):
        return slice(h * HEAD_DIM, (h + 1) * HEAD_DIM)

    line = lax.broadcasted_iota(jnp.int32, (8, LANES), 0)
    for r in range(1, n_inst):
        target = inst(r)
        slot_bias = []
        for m in range(MOST):
            chosen, occupied, seen = jnp.int32(0), jnp.int32(0), jnp.int32(0)
            for i in range(moves):
                hit = (dest_ref[0, i] == target).astype(jnp.int32)
                here = hit * (seen == m).astype(jnp.int32)
                chosen = chosen + here * page_ref[0, i]
                occupied = occupied + here
                seen = seen + hit
            for h, w in spots:
                st_mov[r - 1, h, w, m * page_rows:(m + 1) * page_rows, :] = pool_ref[chosen, :, w, columns_of(h)]
            slot_bias.append(jnp.where(occupied > 0, 0.0, NEG_LARGE))
        row = jnp.full((8, LANES), slot_bias[0], jnp.float32)
        for m in range(1, MOST):
            row = jnp.where(line == m, slot_bias[m], row)
        st_occ[r - 1] = row
    for j in range(table):
        for h, w in spots:
            st_res[h, w, j * page_rows:(j + 1) * page_rows, :] = pool_ref[table_ref[0, j], :, w, columns_of(h)]
    for h, w in spots:
        st_new[h, w] = fresh_ref[:, w, columns_of(h)]
    st_len[...] = jnp.full(st_len.shape, len_ref[0, 0], jnp.int32)
    len_all[a] = st_len[...]
    for h in range(heads):
        q_turned[:, h * queries:(h + 1) * queries] = q_ref[:, h * HEAD_DIM:(h + 1) * HEAD_DIM].T

    pl.semaphore_wait(barrier, len(partners) + share - 1)

    def remote(src, dst, ss, rs, ba, aa):
        return pltpu.make_async_remote_copy(
            src_ref=src, dst_ref=dst, send_sem=ss, recv_sem=rs,
            device_id={"ba": ba, "aa": aa}, device_id_type=MESH,
        )

    sent = []

    def start(*args):
        c = remote(*args)
        c.start()
        sent.append(c)

    for r in range(1, n_inst):
        for j in range(kv_heads):
            to = at_head(j)
            h = lax.rem(mine + j, kv_heads)
            start(st_mov.at[r - 1, h], kv_mov.at[r - 1, member, mine], s_mov.at[r - 1, j], r_mov.at[r - 1, j], inst(r), to)
            start(st_occ.at[r - 1], occ_all.at[r - 1, member, mine], s_occ.at[r - 1, j], r_occ.at[r - 1, j], inst(r), to)
        if r == 1:
            for j in range(1, kv_heads):
                to = at_head(j)
                h = lax.rem(mine + j, kv_heads)
                start(st_new.at[h], kv_new.at[a], s_new.at[j], r_new.at[j], b, to)
                start(st_len, len_all.at[a], s_len.at[j], r_len.at[j], b, to)
                start(st_res.at[h], kv_res.at[a], s_res.at[j], r_res.at[j], b, to)
            for k in range(1, share):
                to = peer(k)
                start(st_new.at[mine], kv_new.at[a], fs_new.at[k - 1, 0], fr_new.at[k - 1, 0], b, to)
                start(st_len, len_all.at[a], fs_len.at[k - 1, 0], fr_len.at[k - 1, 0], b, to)
                start(st_res.at[mine], kv_res.at[a], fs_res.at[k - 1, 0], fr_res.at[k - 1, 0], b, to)
    own_new = pltpu.make_async_copy(st_new.at[mine], kv_new.at[a], l_new)
    own_new.start()
    own_res = pltpu.make_async_copy(st_res.at[mine], kv_res.at[a], l_res)
    own_res.start()

    def arrived(slot, rs, ss):
        remote(slot, slot, ss, rs, b, a).wait_recv()

    def relay(slot, rs, ss, fs, fr, j):
        arrived(slot, rs, ss)
        for k in range(1, share):
            start(slot, slot, fs.at[k - 1, j], fr.at[k - 1, j], b, peer(k))

    def peers_done(buf, fs, fr, first=0):
        for k in range(1, share):
            for j in range(kv_heads):
                src = lax.rem(mine - j + kv_heads, kv_heads) * share + lax.rem(member - k + share, share)
                arrived(buf.at[src], fr.at[k - 1, j], fs.at[k - 1, j])

    for j in range(1, kv_heads):
        src = at_head(-j)
        relay(kv_new.at[src], r_new.at[j], s_new.at[j], fs_new, fr_new, j)
        relay(len_all.at[src], r_len.at[j], s_len.at[j], fs_len, fr_len, j)
        relay(kv_res.at[src], r_res.at[j], s_res.at[j], fs_res, fr_res, j)

    scale = math.log2(math.e) / math.sqrt(HEAD_DIM)

    def attend(keys, values, bias, first):
        turned = values.T
        copies = BLOCK // bias.shape[1]
        wide = jnp.concatenate([bias] * copies, axis=1) if copies > 1 else bias
        for start_at in range(0, heads * queries, BLOCK):
            block = slice(start_at, start_at + BLOCK)
            s = jnp.dot(keys, q_turned[:, block], preferred_element_type=jnp.float32)
            s = s * scale + wide
            top = jnp.max(s, axis=0, keepdims=True)
            if not first:
                old = run_max[:, block]
                top = jnp.maximum(old, top)
            w = jnp.exp2(s - top)
            total = jnp.sum(w, axis=0, keepdims=True)
            high = w.astype(jnp.bfloat16)
            low = (w - high.astype(jnp.float32)).astype(jnp.bfloat16)
            out = jnp.dot(turned, high, preferred_element_type=jnp.float32)
            out = out + jnp.dot(turned, low, preferred_element_type=jnp.float32)
            if not first:
                shrink = jnp.exp2(old - top)
                total = total + run_sum[:, block] * shrink
                out = out + run_out[:, block] * shrink
            run_max[:, block] = top
            run_sum[:, block] = total
            run_out[:, block] = out

    own_new.wait()
    peers_done(kv_new, fs_new, fr_new)
    rows = lax.broadcasted_iota(jnp.int32, (queries, queries), 0)
    columns = lax.broadcasted_iota(jnp.int32, (queries, queries), 1)
    attend(
        kv_new[:, 0].reshape(-1, HEAD_DIM),
        kv_new[:, 1].reshape(-1, HEAD_DIM),
        jnp.where(rows <= columns, 0.0, NEG_LARGE),
        True,
    )
    own_res.wait()
    place = lax.broadcasted_iota(jnp.int32, (table * page_rows, LANES), 0)
    peers_done(len_all, fs_len, fr_len)
    peers_done(kv_res, fs_res, fr_res)
    def attend_resident():
        attend(
            kv_res[:, 0].reshape(-1, HEAD_DIM),
            kv_res[:, 1].reshape(-1, HEAD_DIM),
            jnp.concatenate([jnp.where(place < len_all[i, 0:1, :], 0.0, NEG_LARGE) for i in range(n_aa)], axis=0),
            False,
        )

    far = n_inst - 1

    def back(j):
        return lax.rem(mine - j + kv_heads, kv_heads)

    def other(k):
        return lax.rem(member - k + share, share)

    def relay_moved(r):
        for j in range(kv_heads):
            relay(kv_mov.at[r - 1, member, back(j)], r_mov.at[r - 1, j], s_mov.at[r - 1, j], fs_mov.at[r - 1], fr_mov.at[r - 1], j)
            relay(occ_all.at[r - 1, member, back(j)], r_occ.at[r - 1, j], s_occ.at[r - 1, j], fs_occ.at[r - 1], fr_occ.at[r - 1], j)

    def moved_from(r, k):
        for j in range(kv_heads):
            arrived(kv_mov.at[r - 1, other(k), back(j)], fr_mov.at[r - 1, k - 1, j], fs_mov.at[r - 1, k - 1, j])
            arrived(occ_all.at[r - 1, other(k), back(j)], fr_occ.at[r - 1, k - 1, j], fs_occ.at[r - 1, k - 1, j])

    def attend_moved(r, members):
        attend(
            jnp.concatenate([kv_mov[r - 1, i, :, 0].reshape(-1, HEAD_DIM) for i in members], axis=0),
            jnp.concatenate([kv_mov[r - 1, i, :, 1].reshape(-1, HEAD_DIM) for i in members], axis=0),
            jnp.concatenate([
                jnp.broadcast_to(occ_all[r - 1, i, c, m:m + 1, :], (page_rows, LANES))
                for i in members for c in range(kv_heads) for m in range(MOST)
            ], axis=0),
            False,
        )

    relay_moved(1)
    attend_resident()
    for r in range(1, far):
        if r + 1 < far:
            relay_moved(r + 1)
        for k in range(1, share):
            moved_from(r, k)
        attend_moved(r, range(share))
    if far > 1:
        relay_moved(far)
    attend_moved(far, [member])
    for k in range(1, share):
        moved_from(far, k)
        attend_moved(far, [other(k)])

    def turn(h):
        part = slice(h * queries, (h + 1) * queries)
        return (run_out[:, part] / run_sum[:, part]).T

    for h in range(heads):
        out_ref[:, h * HEAD_DIM:(h + 1) * HEAD_DIM] = turn(h).astype(out_ref.dtype)
    for c in sent:
        c.wait_send()


def local(n_inst, n_aa, queries, new_kv, pool, page_table, ctx_len, move_page, move_dest, append_page):
    pool_pages = pool[0]
    pages, page_rows, _, width = pool_pages.shape
    kv_heads = width // HEAD_DIM
    share = n_aa // kv_heads
    fresh_rows = new_kv[0]
    fresh_count = fresh_rows.shape[0]
    query_count, q_width = queries.shape[1:]
    heads = q_width // HEAD_DIM
    table = page_table.shape[1]
    far = n_inst - 1
    bf, f32 = jnp.bfloat16, jnp.float32
    dma = pltpu.SemaphoreType.DMA
    near = [dma((kv_heads,))] * 4
    attended = pl.pallas_call(
        functools.partial(kernel, n_inst, n_aa, kv_heads),
        out_shape=jax.ShapeDtypeStruct((query_count, q_width), bf),
        in_specs=[pl.BlockSpec(memory_space=pltpu.SMEM)] * 4 + [pl.BlockSpec(memory_space=pltpu.VMEM)] * 3,
        out_specs=pl.BlockSpec(memory_space=pltpu.VMEM),
        scratch_shapes=[
            pltpu.VMEM((kv_heads, 2, table * page_rows, HEAD_DIM), bf),
            pltpu.VMEM((kv_heads, 2, fresh_count, HEAD_DIM), bf),
            pltpu.VMEM((far, kv_heads, 2, MOST * page_rows, HEAD_DIM), bf),
            pltpu.VMEM((8, LANES), jnp.int32),
            pltpu.VMEM((far, 8, LANES), f32),
            pltpu.VMEM((n_aa, 2, table * page_rows, HEAD_DIM), bf),
            pltpu.VMEM((n_aa, 2, fresh_count, HEAD_DIM), bf),
            pltpu.VMEM((far, share, kv_heads, 2, MOST * page_rows, HEAD_DIM), bf),
            pltpu.VMEM((n_aa, 8, LANES), jnp.int32),
            pltpu.VMEM((far, share, kv_heads, 8, LANES), f32),
            pltpu.VMEM((1, heads * query_count), f32),
            pltpu.VMEM((1, heads * query_count), f32),
            pltpu.VMEM((HEAD_DIM, heads * query_count), f32),
            pltpu.VMEM((HEAD_DIM, heads * query_count), bf),
            *near,
            dma((far, kv_heads)), dma((far, kv_heads)),
            dma((kv_heads,)), dma((kv_heads,)),
            dma((far, kv_heads)), dma((far, kv_heads)),
            *([dma((share - 1, kv_heads))] * 4),
            dma((far, share - 1, kv_heads)), dma((far, share - 1, kv_heads)),
            dma((share - 1, kv_heads)), dma((share - 1, kv_heads)),
            dma((far, share - 1, kv_heads)), dma((far, share - 1, kv_heads)),
            dma, dma,
        ],
        compiler_params=pltpu.CompilerParams(collective_id=0, has_side_effects=True),
        name="paged_attention",
    )(page_table, ctx_len, move_page, move_dest, queries[0], pool_pages, fresh_rows)
    zero = jnp.zeros((), jnp.int32)
    updated = lax.dynamic_update_slice(pool_pages, fresh_rows[None], (append_page[0, 0], zero, zero, zero))
    return (attended[None], updated[None])


def solution(mesh):
    return jax.shard_map(
        functools.partial(local, mesh.shape["ba"], mesh.shape["aa"]),
        mesh=mesh,
        in_specs=(
            P("ba", None, "aa"),
            P("ba", "aa", None, None),
            P("ba", "aa", None, None, None),
            P("ba", "aa"),
            P("ba", "aa"),
            P("ba", "aa"),
            P("ba", "aa"),
            P("ba", "aa"),
        ),
        out_specs=(P("ba", None, "aa"), P("ba", "aa", None, None, None)),
        check_vma=False,
    )
```

```python
import functools
import math

import jax
import jax.numpy as jnp
from jax import lax
from jax.experimental import pallas as pl
from jax.experimental.pallas import tpu as pltpu
from jax.sharding import PartitionSpec as P

HEAD_DIM = 128
MOST = 2
LANES = 128
BLOCK = 256
NEG_LARGE = -1e30
MESH = pl.DeviceIdType.MESH


def kernel(
    n_inst, n_aa, kv_heads,
    table_ref, len_ref, page_ref, dest_ref, q_ref, pool_ref, fresh_ref,
    out_ref,
    st_res, st_new, st_mov, st_len, st_occ,
    kv_res, kv_new, kv_mov, len_all, occ_all,
    run_max, run_sum, run_out, q_turned,
    s_res, r_res, s_new, r_new, s_mov, r_mov, s_len, r_len, s_occ, r_occ,
    fs_res, fr_res, fs_new, fr_new, fs_mov, fr_mov, fs_len, fr_len, fs_occ, fr_occ,
    l_new, l_res,
):
    b = lax.axis_index("ba")
    a = lax.axis_index("aa")
    share = n_aa // kv_heads
    mine, member = a // share, a % share
    table = table_ref.shape[1]
    moves = page_ref.shape[1]
    page_rows = pool_ref.shape[1]
    queries = q_ref.shape[0]
    heads = q_ref.shape[1] // HEAD_DIM

    def inst(r):
        return lax.rem(b + r + n_inst, n_inst)

    def at_head(j):
        return lax.rem(mine + j + kv_heads, kv_heads) * share + member

    def peer(k):
        return mine * share + lax.rem(member + k + share, share)

    barrier = pltpu.get_barrier_semaphore()
    partners = [(r, j) for r in range(n_inst) for j in range(kv_heads) if r or j]
    for r, j in partners:
        pl.semaphore_signal(barrier, inc=1, device_id={"ba": inst(r), "aa": at_head(j)}, device_id_type=MESH)
    for k in range(1, share):
        pl.semaphore_signal(barrier, inc=1, device_id={"ba": b, "aa": peer(k)}, device_id_type=MESH)

    spots = [(h, w) for h in range(kv_heads) for w in range(2)]

    def columns_of(h):
        return slice(h * HEAD_DIM, (h + 1) * HEAD_DIM)

    line = lax.broadcasted_iota(jnp.int32, (8, LANES), 0)
    for r in range(1, n_inst):
        target = inst(r)
        slot_bias = []
        for m in range(MOST):
            chosen, occupied, seen = jnp.int32(0), jnp.int32(0), jnp.int32(0)
            for i in range(moves):
                hit = (dest_ref[0, i] == target).astype(jnp.int32)
                here = hit * (seen == m).astype(jnp.int32)
                chosen = chosen + here * page_ref[0, i]
                occupied = occupied + here
                seen = seen + hit
            for h, w in spots:
                st_mov[r - 1, h, w, m * page_rows:(m + 1) * page_rows, :] = pool_ref[chosen, :, w, columns_of(h)]
            slot_bias.append(jnp.where(occupied > 0, 0.0, NEG_LARGE))
        row = jnp.full((8, LANES), slot_bias[0], jnp.float32)
        for m in range(1, MOST):
            row = jnp.where(line == m, slot_bias[m], row)
        st_occ[r - 1] = row
    for j in range(table):
        for h, w in spots:
            st_res[h, w, j * page_rows:(j + 1) * page_rows, :] = pool_ref[table_ref[0, j], :, w, columns_of(h)]
    for h, w in spots:
        st_new[h, w] = fresh_ref[:, w, columns_of(h)]
    st_len[...] = jnp.full(st_len.shape, len_ref[0, 0], jnp.int32)
    len_all[a] = st_len[...]
    for h in range(heads):
        q_turned[:, h * queries:(h + 1) * queries] = q_ref[:, h * HEAD_DIM:(h + 1) * HEAD_DIM].T

    pl.semaphore_wait(barrier, len(partners) + share - 1)

    def remote(src, dst, ss, rs, ba, aa):
        return pltpu.make_async_remote_copy(
            src_ref=src, dst_ref=dst, send_sem=ss, recv_sem=rs,
            device_id={"ba": ba, "aa": aa}, device_id_type=MESH,
        )

    sent = []

    def start(*args):
        c = remote(*args)
        c.start()
        sent.append(c)

    for r in range(1, n_inst):
        for j in range(kv_heads):
            to = at_head(j)
            h = lax.rem(mine + j, kv_heads)
            start(st_mov.at[r - 1, h], kv_mov.at[r - 1, member, mine], s_mov.at[r - 1, j], r_mov.at[r - 1, j], inst(r), to)
            start(st_occ.at[r - 1], occ_all.at[r - 1, member, mine], s_occ.at[r - 1, j], r_occ.at[r - 1, j], inst(r), to)
        if r == 1:
            for j in range(1, kv_heads):
                to = at_head(j)
                h = lax.rem(mine + j, kv_heads)
                start(st_new.at[h], kv_new.at[a], s_new.at[j], r_new.at[j], b, to)
                start(st_len, len_all.at[a], s_len.at[j], r_len.at[j], b, to)
                start(st_res.at[h], kv_res.at[a], s_res.at[j], r_res.at[j], b, to)
            for k in range(1, share):
                to = peer(k)
                start(st_new.at[mine], kv_new.at[a], fs_new.at[k - 1, 0], fr_new.at[k - 1, 0], b, to)
                start(st_len, len_all.at[a], fs_len.at[k - 1, 0], fr_len.at[k - 1, 0], b, to)
                start(st_res.at[mine], kv_res.at[a], fs_res.at[k - 1, 0], fr_res.at[k - 1, 0], b, to)
    own_new = pltpu.make_async_copy(st_new.at[mine], kv_new.at[a], l_new)
    own_new.start()
    own_res = pltpu.make_async_copy(st_res.at[mine], kv_res.at[a], l_res)
    own_res.start()

    def arrived(slot, rs, ss):
        remote(slot, slot, ss, rs, b, a).wait_recv()

    def relay(slot, rs, ss, fs, fr, j):
        arrived(slot, rs, ss)
        for k in range(1, share):
            start(slot, slot, fs.at[k - 1, j], fr.at[k - 1, j], b, peer(k))

    def peers_done(buf, fs, fr, first=0):
        for k in range(1, share):
            for j in range(kv_heads):
                src = lax.rem(mine - j + kv_heads, kv_heads) * share + lax.rem(member - k + share, share)
                arrived(buf.at[src], fr.at[k - 1, j], fs.at[k - 1, j])

    for j in range(1, kv_heads):
        src = at_head(-j)
        relay(kv_new.at[src], r_new.at[j], s_new.at[j], fs_new, fr_new, j)
        relay(len_all.at[src], r_len.at[j], s_len.at[j], fs_len, fr_len, j)
        relay(kv_res.at[src], r_res.at[j], s_res.at[j], fs_res, fr_res, j)

    scale = math.log2(math.e) / math.sqrt(HEAD_DIM)

    def attend(keys, values, bias, first):
        turned = values.T
        copies = BLOCK // bias.shape[1]
        wide = jnp.concatenate([bias] * copies, axis=1) if copies > 1 else bias
        for start_at in range(0, heads * queries, BLOCK):
            block = slice(start_at, start_at + BLOCK)
            s = jnp.dot(keys, q_turned[:, block], preferred_element_type=jnp.float32)
            s = s * scale + wide
            top = jnp.max(s, axis=0, keepdims=True)
            if not first:
                old = run_max[:, block]
                top = jnp.maximum(old, top)
            w = jnp.exp2(s - top)
            total = jnp.sum(w, axis=0, keepdims=True)
            high = w.astype(jnp.bfloat16)
            low = (w - high.astype(jnp.float32)).astype(jnp.bfloat16)
            out = jnp.dot(turned, high, preferred_element_type=jnp.float32)
            out = out + jnp.dot(turned, low, preferred_element_type=jnp.float32)
            if not first:
                shrink = jnp.exp2(old - top)
                total = total + run_sum[:, block] * shrink
                out = out + run_out[:, block] * shrink
            run_max[:, block] = top
            run_sum[:, block] = total
            run_out[:, block] = out

    own_new.wait()
    peers_done(kv_new, fs_new, fr_new)
    rows = lax.broadcasted_iota(jnp.int32, (queries, queries), 0)
    columns = lax.broadcasted_iota(jnp.int32, (queries, queries), 1)
    attend(
        kv_new[:, 0].reshape(-1, HEAD_DIM),
        kv_new[:, 1].reshape(-1, HEAD_DIM),
        jnp.where(rows <= columns, 0.0, NEG_LARGE),
        True,
    )
    own_res.wait()
    place = lax.broadcasted_iota(jnp.int32, (table * page_rows, LANES), 0)
    peers_done(len_all, fs_len, fr_len)
    peers_done(kv_res, fs_res, fr_res)
    def attend_resident():
        attend(
            kv_res[:, 0].reshape(-1, HEAD_DIM),
            kv_res[:, 1].reshape(-1, HEAD_DIM),
            jnp.concatenate([jnp.where(place < len_all[i, 0:1, :], 0.0, NEG_LARGE) for i in range(n_aa)], axis=0),
            False,
        )

    far = n_inst - 1

    def back(j):
        return lax.rem(mine - j + kv_heads, kv_heads)

    def other(k):
        return lax.rem(member - k + share, share)

    def relay_moved(r):
        for j in range(kv_heads):
            relay(kv_mov.at[r - 1, member, back(j)], r_mov.at[r - 1, j], s_mov.at[r - 1, j], fs_mov.at[r - 1], fr_mov.at[r - 1], j)
            relay(occ_all.at[r - 1, member, back(j)], r_occ.at[r - 1, j], s_occ.at[r - 1, j], fs_occ.at[r - 1], fr_occ.at[r - 1], j)

    def moved_from(r, k):
        for j in range(kv_heads):
            arrived(kv_mov.at[r - 1, other(k), back(j)], fr_mov.at[r - 1, k - 1, j], fs_mov.at[r - 1, k - 1, j])
            arrived(occ_all.at[r - 1, other(k), back(j)], fr_occ.at[r - 1, k - 1, j], fs_occ.at[r - 1, k - 1, j])

    def attend_moved(r, members):
        attend(
            jnp.concatenate([kv_mov[r - 1, i, :, 0].reshape(-1, HEAD_DIM) for i in members], axis=0),
            jnp.concatenate([kv_mov[r - 1, i, :, 1].reshape(-1, HEAD_DIM) for i in members], axis=0),
            jnp.concatenate([
                jnp.broadcast_to(occ_all[r - 1, i, c, m:m + 1, :], (page_rows, LANES))
                for i in members for c in range(kv_heads) for m in range(MOST)
            ], axis=0),
            False,
        )

    relay_moved(1)
    attend_resident()
    for r in range(1, far):
        if r + 1 < far:
            relay_moved(r + 1)
        for k in range(1, share):
            moved_from(r, k)
        attend_moved(r, range(share))
    if far > 1:
        relay_moved(far)
    attend_moved(far, [member])
    for k in range(1, share):
        moved_from(far, k)
        attend_moved(far, [other(k)])

    def turn(h):
        part = slice(h * queries, (h + 1) * queries)
        return (run_out[:, part] / run_sum[:, part]).T

    for h in range(heads):
        out_ref[:, h * HEAD_DIM:(h + 1) * HEAD_DIM] = turn(h).astype(out_ref.dtype)
    for c in sent:
        c.wait_send()


def finish(append_ref, rows_ref, pool_ref, fresh_ref, out_ref, updated_ref):
    out_ref[...] = rows_ref[...]
    updated_ref[...] = pool_ref[...]
    updated_ref[append_ref[0, 0], 0:fresh_ref.shape[0]] = fresh_ref[...]


def local(n_inst, n_aa, queries, new_kv, pool, page_table, ctx_len, move_page, move_dest, append_page):
    pool_pages = pool[0]
    pages, page_rows, _, width = pool_pages.shape
    kv_heads = width // HEAD_DIM
    share = n_aa // kv_heads
    fresh_rows = new_kv[0]
    fresh_count = fresh_rows.shape[0]
    query_count, q_width = queries.shape[1:]
    heads = q_width // HEAD_DIM
    table = page_table.shape[1]
    far = n_inst - 1
    bf, f32 = jnp.bfloat16, jnp.float32
    dma = pltpu.SemaphoreType.DMA
    near = [dma((kv_heads,))] * 4
    attended = pl.pallas_call(
        functools.partial(kernel, n_inst, n_aa, kv_heads),
        out_shape=jax.ShapeDtypeStruct((query_count, q_width), bf),
        in_specs=[pl.BlockSpec(memory_space=pltpu.SMEM)] * 4 + [pl.BlockSpec(memory_space=pltpu.VMEM)] * 3,
        out_specs=pl.BlockSpec(memory_space=pltpu.VMEM),
        scratch_shapes=[
            pltpu.VMEM((kv_heads, 2, table * page_rows, HEAD_DIM), bf),
            pltpu.VMEM((kv_heads, 2, fresh_count, HEAD_DIM), bf),
            pltpu.VMEM((far, kv_heads, 2, MOST * page_rows, HEAD_DIM), bf),
            pltpu.VMEM((8, LANES), jnp.int32),
            pltpu.VMEM((far, 8, LANES), f32),
            pltpu.VMEM((n_aa, 2, table * page_rows, HEAD_DIM), bf),
            pltpu.VMEM((n_aa, 2, fresh_count, HEAD_DIM), bf),
            pltpu.VMEM((far, share, kv_heads, 2, MOST * page_rows, HEAD_DIM), bf),
            pltpu.VMEM((n_aa, 8, LANES), jnp.int32),
            pltpu.VMEM((far, share, kv_heads, 8, LANES), f32),
            pltpu.VMEM((1, heads * query_count), f32),
            pltpu.VMEM((1, heads * query_count), f32),
            pltpu.VMEM((HEAD_DIM, heads * query_count), f32),
            pltpu.VMEM((HEAD_DIM, heads * query_count), bf),
            *near,
            dma((far, kv_heads)), dma((far, kv_heads)),
            dma((kv_heads,)), dma((kv_heads,)),
            dma((far, kv_heads)), dma((far, kv_heads)),
            *([dma((share - 1, kv_heads))] * 4),
            dma((far, share - 1, kv_heads)), dma((far, share - 1, kv_heads)),
            dma((share - 1, kv_heads)), dma((share - 1, kv_heads)),
            dma((far, share - 1, kv_heads)), dma((far, share - 1, kv_heads)),
            dma, dma,
        ],
        compiler_params=pltpu.CompilerParams(collective_id=0, has_side_effects=True, vmem_limit_bytes=32 * 2**20),
        name="paged_attention",
    )(page_table, ctx_len, move_page, move_dest, queries[0], pool_pages, fresh_rows)
    attended, updated = pl.pallas_call(
        finish,
        out_shape=(
            jax.ShapeDtypeStruct(attended.shape, bf),
            jax.ShapeDtypeStruct(pool_pages.shape, bf),
        ),
        in_specs=[pl.BlockSpec(memory_space=pltpu.SMEM)] + [pl.BlockSpec(memory_space=pltpu.VMEM)] * 3,
        out_specs=(pl.BlockSpec(memory_space=pltpu.VMEM),) * 2,
        compiler_params=pltpu.CompilerParams(vmem_limit_bytes=12 * 2**20),
        name="finish",
    )(append_page, attended, pool_pages, fresh_rows)
    return (attended[None], updated[None])


def solution(mesh):
    return jax.shard_map(
        functools.partial(local, mesh.shape["ba"], mesh.shape["aa"]),
        mesh=mesh,
        in_specs=(
            P("ba", None, "aa"),
            P("ba", "aa", None, None),
            P("ba", "aa", None, None, None),
            P("ba", "aa"),
            P("ba", "aa"),
            P("ba", "aa"),
            P("ba", "aa"),
            P("ba", "aa"),
        ),
        out_specs=(P("ba", None, "aa"), P("ba", "aa", None, None, None)),
        check_vma=False,
    )
```
